32 devices in a mesh: blk: 4 (over y, core), grp: 8 (over z, x).
Axes of the slice: x: 2, y: 2, z: 4, core: 2. Of those that a mesh axis runs over, the one named last changes fastest.
Arguments:
- gas_state: bfloat16 [16, 32, 32768], P(None, None, ('grp', 'blk')), may hold values from -6 to 6
- cos_zenith: bfloat16 [32768], P(('grp', 'blk')), may hold values from 0.049804688 to 1
- daylit: int32 [32768], P(('grp', 'blk')), may hold values from 0 to 1
- fine_area: float32 [131072], P(('grp', 'blk')), may hold values from 0.25 to 4
- fine_albedo: float32 [2, 131072], P(None, ('grp', 'blk')), may hold values from 0.05 to 0.85
- parent_of: int32 [131072], P(('grp', 'blk')), may hold values from 0 to 4095, as said below
- optics_weight: bfloat16 [64, 16], replicated, may hold values from -1.5 to 1.5
- solar_weight: float32 [32], replicated, may hold values from 0.01 to 0.1
- neighbours: int32 [3, 32768], P(None, ('grp', 'blk')), may hold values from 0 to 32767, as said below
- side_weight: float32 [3, 32768], P(None, ('grp', 'blk')), may hold values from 0.05 to 0.3
Outputs:
- fluxes: float32 [2, 33, 32768], P(None, None, ('grp', 'blk'))
The draws below stay inside these ranges and needn't reach their ends.
Inputs may be any that keep to these rules, and one draw needn't show every extreme that they name: `parent_of`: the fine cells of one index of grp have their parents among that index's columns, numbered from 0 within it; each column has exactly 4 fine cells, and the 128 fine cells of an aligned block share 128 // 4 consecutive columns. `neighbours`: every neighbour lies within 128 columns of its column and among the columns of the same index of grp; a neighbour may be the column itself.
All inputs are finite; a program needn't handle non-finite values.
Results may differ from the reference program's by a relative error of at most 0.0003.
Values may be sent and summed in bfloat16 or wider, within the bound.
A program may use at most 64 MiB of HBM per device.

```python
import math
import jax
import jax.numpy as jnp
from jax import lax

G = 32
F = 16
LEV = 32
COLS_DEV = 1024
CB = 128
KIDS = 4
FB = 128
REACH = 128
GROUP_COLS = 4096
COLUMNS = 32768
FINE = 131072
N_BLK = 4
N_GRP = 8


def draw_daylit(key, part):
    devices = N_GRP * N_BLK
    nblocks = COLS_DEV // CB
    key_one, key_two, key_three = jax.random.split(jax.random.fold_in(key, 11), 3)
    blk_place = jnp.arange(devices, dtype=jnp.int32) % N_BLK
    trend = blk_place * nblocks // max(N_BLK - 1, 1)
    jitter = jax.random.randint(key_one, (devices,), -(nblocks // 2), nblocks // 2 + 1)
    lit_blocks = jnp.clip(trend + jitter, 0, nblocks)
    scores = jax.random.randint(key_two, (devices, nblocks), 0, 1 << 16) * nblocks + jnp.arange(nblocks, dtype=jnp.int32)[None, :]
    ordering = jnp.argsort(scores, axis=1)
    ranking = jnp.argsort(ordering, axis=1)
    partial_len = jax.random.randint(key_three, (devices, 1, 1), 1, CB)
    inside = jnp.arange(CB, dtype=jnp.int32)[None, None, :]
    fully = ranking[:, :, None] < lit_blocks[:, None, None]
    border = (ranking[:, :, None] == lit_blocks[:, None, None]) & (inside < partial_len)
    return (fully | border).astype(jnp.int32).reshape(COLUMNS)


def draw_parent_of(key, part):
    per_span = FB // KIDS
    spans = GROUP_COLS // per_span
    key_one, key_two = jax.random.split(jax.random.fold_in(key, 23))
    scores = jax.random.randint(key_one, (N_GRP, spans), 0, 1 << 12) * spans + jnp.arange(spans, dtype=jnp.int32)[None, :]
    span_order = jnp.argsort(scores, axis=1).astype(jnp.int32)
    inner_scores = jax.random.randint(key_two, (N_GRP, spans, FB), 0, 1 << 16) * FB + jnp.arange(FB, dtype=jnp.int32)[None, None, :]
    inner = jnp.argsort(inner_scores, axis=2).astype(jnp.int32) % per_span
    parent = span_order[:, :, None] * per_span + inner
    return parent.reshape(FINE).astype(jnp.int32)


def draw_neighbours(key, part):
    column = jnp.arange(COLUMNS, dtype=jnp.int32)
    lower = column // GROUP_COLS * GROUP_COLS
    offsets = jax.random.randint(jax.random.fold_in(key, 37), (3, COLUMNS), -REACH, REACH + 1)
    return jnp.clip(column[None, :] + offsets, lower[None, :], lower[None, :] + GROUP_COLS - 1).astype(jnp.int32)


def block_scale(key, dims, shards, low, top_value):
    def one(axis_at, blocks):
        draws = jax.random.uniform(jax.random.fold_in(jax.random.fold_in(key, 6), axis_at), (blocks,), jnp.float32, low / len(shards), top_value / len(shards))
        return jnp.repeat(jnp.exp(draws), dims[axis_at] // blocks).reshape((-1,) + (1,) * (len(dims) - axis_at - 1))

    gain = one(*shards[0])
    for cut in shards[1:]:
        gain = gain * one(*cut)
    return gain


def bell_draw(own_key, extent, scale, bound, shards=(), kind=jnp.bfloat16):
    values = scale * jax.random.normal(own_key, extent, jnp.float32)
    if shards:
        values = values * block_scale(own_key, extent, shards, -0.22, 0.18)
    return jnp.clip(values, -bound, bound).astype(kind)


def setup_inputs(seed: int = 0) -> dict:
    seeds = jax.random.split(jax.random.key(seed), 11)
    gas_state = bell_draw(seeds[0], (F, LEV, COLUMNS), 1.0, 6.0, ((2, 32),))
    cos_zenith = jnp.clip(0.049804688 + 0.9501953 * jax.random.uniform(seeds[1], (COLUMNS,), jnp.float32) ** block_scale(seeds[1], (COLUMNS,), ((0, 32),), -0.2, 0.2), 0.049804688, 1.0).astype(jnp.bfloat16)
    daylit = draw_daylit(jax.random.fold_in(seeds[10], 71), 0)
    fine_area = jnp.clip(jnp.exp(math.log(4.0) - 2.7725887 * jax.random.uniform(seeds[3], (FINE,), jnp.float32) ** block_scale(seeds[3], (FINE,), ((0, 32),), -0.2, 0.2)), 0.25, 4.0)
    fine_albedo = jnp.clip(0.05 + 0.8 * jax.random.uniform(seeds[4], (2, FINE), jnp.float32) ** block_scale(seeds[4], (2, FINE), ((1, 32),), -0.2, 0.2), 0.05, 0.85)
    parent_of = draw_parent_of(jax.random.fold_in(seeds[10], 71), 0)
    optics_weight = bell_draw(seeds[6], (2 * G, F), F ** -0.5, 1.5)
    solar_weight = jnp.clip(jnp.exp(jax.random.uniform(seeds[7], (G,), jnp.float32, math.log(0.01), math.log(0.1))), 0.01, 0.1)
    neighbours = draw_neighbours(jax.random.fold_in(seeds[10], 71), 0)
    side_weight = jnp.clip(0.05 + 0.25 * jax.random.uniform(seeds[9], (3, COLUMNS), jnp.float32) ** block_scale(seeds[9], (3, COLUMNS), ((1, 32),), -0.2, 0.2), 0.05, 0.3)
    return dict(gas_state=gas_state, cos_zenith=cos_zenith, daylit=daylit, fine_area=fine_area, fine_albedo=fine_albedo, parent_of=parent_of, optics_weight=optics_weight, solar_weight=solar_weight, neighbours=neighbours, side_weight=side_weight)


ASYM = 0.8
TAU_SCALE = 0.08
SSA_MAX = 0.98

def column_fluxes(optics_mix, cosine_col, albedo_direct, albedo_diffuse, lit_flag, solar_weight):
    gpoints = solar_weight.shape[0]
    width = cosine_col.shape[0]
    optical_depth = TAU_SCALE * jax.nn.softplus(optics_mix[:, :gpoints])
    single_albedo = SSA_MAX * jax.nn.sigmoid(optics_mix[:, gpoints:])
    slant = cosine_col[None, None, :]
    direct_share = jnp.exp(-optical_depth / slant)
    gamma_one = 2.0 - single_albedo * (1.25 + 0.75 * ASYM)
    gamma_two = 0.75 * single_albedo * (1.0 - ASYM)
    eigen_rate = jnp.sqrt((gamma_one - gamma_two) * (gamma_one + gamma_two))
    damping = jnp.exp(-eigen_rate * optical_depth)
    damped_sq = damping * damping
    divisor = eigen_rate + gamma_one + (eigen_rate - gamma_one) * damped_sq
    reflect = gamma_two * (1.0 - damped_sq) / divisor
    transmit = 2.0 * eigen_rate * damping / divisor
    back_share = 0.5 * (1.0 - ASYM * slant)
    scattered = single_albedo * (1.0 - direct_share)
    rising = scattered * back_share
    falling = scattered - rising
    top_flux = solar_weight[:, None] * cosine_col[None, :]
    direct = top_flux[None] * jnp.concatenate([jnp.ones_like(top_flux)[None], jnp.cumprod(direct_share, axis=0)], axis=0)

    def ascend(carry, layer):
        albedo, source = carry
        inverse = 1.0 / (1.0 - albedo * layer[0])
        new_albedo = layer[0] + layer[1] * layer[1] * albedo * inverse
        new_source = layer[2] * layer[4] + layer[1] * (source + albedo * layer[3] * layer[4]) * inverse
        return ((new_albedo, new_source), (albedo, source, inverse))
    ground = (jnp.broadcast_to(albedo_diffuse[None, :], top_flux.shape), albedo_direct[None, :] * direct[-1])
    (top_albedo, source_top), below = lax.scan(ascend, ground, (reflect, transmit, rising, falling, direct[:-1]), reverse=True)

    def descend(diffuse, layer):
        updated = (layer[1] * diffuse + layer[0] * layer[6] + layer[3] * layer[4]) * layer[7]
        return (updated, (updated, layer[5] * updated + layer[6]))
    last_diffuse, (diffuse_down, diffuse_up) = lax.scan(descend, jnp.zeros_like(top_flux), (reflect, transmit, rising, falling, direct[:-1], below[0], below[1], below[2]))
    first_row = jnp.zeros((1, width), jnp.float32)
    downward = lax.optimization_barrier(jnp.sum(direct, axis=1)) + jnp.concatenate([first_row, lax.optimization_barrier(jnp.sum(diffuse_down, axis=1))], axis=0)
    upward = jnp.concatenate([lax.optimization_barrier(jnp.sum(source_top, axis=0))[None], lax.optimization_barrier(jnp.sum(diffuse_up, axis=1))], axis=0)
    return jnp.stack([downward, upward]) * lit_flag[None, None, :]

def reference(gas_state, cos_zenith, daylit, fine_area, fine_albedo, parent_of, optics_weight, solar_weight, neighbours, side_weight):
    weights = jnp.stack([fine_area, fine_area * fine_albedo[0], fine_area * fine_albedo[1]])
    fine_group = (jnp.arange(FINE, dtype=jnp.int32) // (KIDS * GROUP_COLS)).astype(jnp.int32)
    parent_global = (parent_of + fine_group * GROUP_COLS).astype(jnp.int32)
    totals = jax.vmap(lambda values: jax.ops.segment_sum(values, parent_global, num_segments=COLUMNS))(weights)
    albedo = (totals[1:] / totals[0]).astype(jnp.bfloat16).astype(jnp.float32)
    cosine_all = cos_zenith.astype(jnp.float32)
    lit_all = daylit.astype(jnp.float32)
    matrix = optics_weight.astype(jnp.float32)
    nblocks = COLUMNS // COLS_DEV

    def one_block(number):
        begin_at = (number * COLS_DEV).astype(jnp.int32)
        inputs = lax.dynamic_slice_in_dim(gas_state, begin_at, COLS_DEV, 2).astype(jnp.float32)
        optics_mix = jnp.einsum('gf,fln->lgn', matrix, inputs, precision=lax.Precision.HIGHEST)
        cosine_col = lax.dynamic_slice_in_dim(cosine_all, begin_at, COLS_DEV, 0)
        albedo_cols = lax.dynamic_slice_in_dim(albedo, begin_at, COLS_DEV, 1)
        lit_cols = lax.dynamic_slice_in_dim(lit_all, begin_at, COLS_DEV, 0)
        return column_fluxes(optics_mix, cosine_col, albedo_cols[0], albedo_cols[1], lit_cols, solar_weight)
    stacked = lax.map(one_block, jnp.arange(nblocks, dtype=jnp.int32))
    column_flux = jnp.moveaxis(stacked, 0, 2).reshape(2, LEV + 1, COLUMNS)
    result = column_flux
    for index_k in range(3):
        beside = jnp.take(column_flux, neighbours[index_k], axis=2)
        result = result + side_weight[index_k][None, None, :] * (beside - column_flux)
    return result
```

```python
import functools

import jax
import jax.numpy as jnp
from jax import lax
from jax.experimental import pallas as pl
from jax.experimental.pallas import tpu as pltpu
from jax.sharding import PartitionSpec as P

CB = 128
FB = 128
ASYM = 0.8
TAU_SCALE = 0.08
SSA_MAX = 0.98
CHUNK = 8
VMEM = pltpu.VMEM


def round_up(value, multiple):
    return -(-value // multiple) * multiple


def local_albedo(area_ref, albedo_ref, parent_ref, span):
    blocks = area_ref.shape[0]
    area = area_ref[...]
    rows = [
        jnp.concatenate([albedo_ref[s : s + 1, b * FB : (b + 1) * FB] for b in range(blocks)], axis=0)
        for s in range(2)
    ]
    weights = [area, area * rows[0], area * rows[1]]
    weights = [jnp.transpose(w) for w in weights]
    parent = jnp.transpose(parent_ref[...])
    inside = parent & (span - 1)
    sums = [[], [], []]
    for j in range(span):
        hit = inside == j
        for q in range(3):
            sums[q].append(jnp.sum(jnp.where(hit, weights[q], 0.0), axis=0, keepdims=True))
    totals = [jnp.concatenate(s, axis=0) for s in sums]
    first = (totals[1] / totals[0]).astype(jnp.bfloat16).astype(jnp.float32)
    second = (totals[2] / totals[0]).astype(jnp.bfloat16).astype(jnp.float32)
    number = (parent[0:1] // span).astype(jnp.float32)
    return first, second, number


def albedo_kernel(span, area_ref, albedo_ref, parent_ref, out_ref):
    blocks = area_ref.shape[0]
    first, second, number = local_albedo(area_ref, albedo_ref, parent_ref, span)
    out_ref[...] = jnp.zeros_like(out_ref)
    out_ref[0:span, 0:blocks] = first
    out_ref[0:span, blocks : 2 * blocks] = second
    out_ref[span : span + 1, 0:blocks] = number


def pick_albedo(pieces, start_span, span, blocks, ncb):
    per = CB // span
    table = jnp.concatenate(
        [jnp.concatenate([p[0:span, s * blocks : (s + 1) * blocks] for p in pieces], axis=1) for s in range(2)],
        axis=0,
    ).astype(jnp.bfloat16)
    number = jnp.concatenate([p[span : span + 1, 0:blocks] for p in pieces], axis=1).astype(jnp.int32)
    total = number.shape[1]
    row = lax.broadcasted_iota(jnp.int32, (ncb, total), 0) * per + start_span
    parts = []
    for m in range(per):
        chosen = (number == row + m).astype(jnp.float32).astype(jnp.bfloat16)
        parts.append(
            lax.dot_general(chosen, table, (((1,), (1,)), ((), ())), preferred_element_type=jnp.float32)
        )
    direct = jnp.concatenate([p[:, 0:span] for p in parts], axis=1)
    diffuse = jnp.concatenate([p[:, span : 2 * span] for p in parts], axis=1)
    return direct, diffuse


def expand_weight(weight_ref, big_ref):
    rows, feats = weight_ref.shape
    half = big_ref.shape[1] // feats
    wide = feats * half
    source = lax.broadcasted_iota(jnp.int32, (feats, wide), 0)
    column = lax.broadcasted_iota(jnp.int32, (feats, wide), 1)
    spread = (column // half == source).astype(jnp.float32).astype(jnp.bfloat16)
    repeated = jnp.dot(weight_ref[...], spread, preferred_element_type=jnp.float32)
    level = lax.broadcasted_iota(jnp.int32, (rows, wide), 1) % half
    for l in range(half):
        big_ref[l * rows : (l + 1) * rows, :] = jnp.where(level == l, repeated, 0.0).astype(jnp.bfloat16)


def layer(mix, gpoints, rate, back, carry):
    direct, big_b, big_q = carry
    x = mix[:gpoints]
    y = mix[gpoints:]
    soft = jnp.maximum(x, 0.0) + jnp.log(1.0 + jnp.exp(-jnp.abs(x)))
    share = jnp.exp(soft * rate)
    th = jnp.tanh(0.5 * y)
    h = 0.5 * SSA_MAX
    w = h + h * th
    up1 = 1.25 + 0.75 * ASYM
    g1 = 2.0 - up1 * w
    c2 = 0.75 * (1.0 - ASYM)
    g2 = c2 * w
    minus = 2.0 - (up1 + c2) * w
    plus = 2.0 - (up1 - c2) * w
    square = minus * plus
    k = square * lax.rsqrt(square)
    q = jnp.exp((k * soft) * (-TAU_SCALE))
    q2 = q * q
    kp = k + g1
    km = k - g1
    d = kp + km * q2
    dd = km + kp * q2
    r = g2 - g2 * q2
    t2 = (k + k) * q
    below = direct * share
    scattered = w * (direct - below)
    rising = scattered * back
    falling = scattered - rising
    z = 1.0 / (d - r * big_b)
    t = t2 * z
    s = (r * big_q + d * rising) * z
    new_b = (r + dd * big_b) * z
    new_q = t * (big_q + big_b * rising) + falling
    return t, s, (below, new_b, new_q)


def solve_block(cb, gas_ref, big_ref, cos_ref, lit_ref, solar, surface, state_ref, flux_ref, up_row):
    feats, lev = gas_ref.shape[0], gas_ref.shape[1]
    gpoints = solar.shape[0]
    rows = 2 * gpoints
    half = big_ref.shape[1] // feats
    cols = pl.ds(pl.multiple_of(cb * CB, CB), CB)
    mu = cos_ref[pl.ds(cb, 1), :]
    lit = lit_ref[pl.ds(cb, 1), :]
    rate = jnp.broadcast_to(-TAU_SCALE / mu, (gpoints, CB))
    back = jnp.broadcast_to(0.5 * (1.0 - ASYM * mu), (gpoints, CB))
    top = solar * mu
    zero = jnp.zeros((gpoints, CB), jnp.float32)
    carry = (top, zero, zero)

    for part in range(lev // half):
        inputs = gas_ref[:, part * half : (part + 1) * half, cols].reshape(feats * half, CB)

        def down(step, carry, part=part, inputs=inputs):
            at = pl.multiple_of(step * (CHUNK * rows), CHUNK * rows)
            mix = jnp.dot(
                big_ref[pl.ds(at, CHUNK * rows), :], inputs, preferred_element_type=jnp.float32
            )
            for i in range(CHUNK):
                level = part * half + step * CHUNK + i
                state_ref[2, level] = carry[1]
                state_ref[3, level] = carry[2] + carry[0]
                t, s, carry = layer(mix[i * rows : (i + 1) * rows], gpoints, rate, back, carry)
                state_ref[0, level] = t
                state_ref[1, level] = s
            return carry

        carry = lax.fori_loop(0, half // CHUNK, down, carry)

    direct, big_b, big_q = carry
    direct_albedo, diffuse_albedo = surface(cb)
    up = (diffuse_albedo * big_q + direct_albedo * direct) / (1.0 - diffuse_albedo * big_b)
    flux_ref[lev : lev + 1, cols] = jnp.sum(big_b * up + big_q + direct, axis=0, keepdims=True) * lit
    flux_ref[up_row + lev : up_row + lev + 1, cols] = jnp.sum(up, axis=0, keepdims=True) * lit

    def back_up(step, up):
        first = pl.multiple_of(lev - CHUNK - step * CHUNK, CHUNK)
        downs, ups = [None] * CHUNK, [None] * CHUNK
        for i in reversed(range(CHUNK)):
            up = state_ref[0, first + i] * up + state_ref[1, first + i]
            down = state_ref[2, first + i] * up + state_ref[3, first + i]
            downs[i] = jnp.sum(down, axis=0, keepdims=True)
            ups[i] = jnp.sum(up, axis=0, keepdims=True)
        flux_ref[pl.ds(first, CHUNK), cols] = jnp.concatenate(downs, axis=0) * lit
        flux_ref[pl.ds(up_row + first, CHUNK), cols] = jnp.concatenate(ups, axis=0) * lit
        return up

    lax.fori_loop(0, lev // CHUNK, back_up, up)


def solar_column(solar_ref):
    row = solar_ref[...]
    n = row.shape[1]
    diagonal = lax.broadcasted_iota(jnp.int32, (n, n), 0) == lax.broadcasted_iota(jnp.int32, (n, n), 1)
    return jnp.sum(jnp.where(diagonal, row, 0.0), axis=1, keepdims=True)


def flux_kernel(
    n, span, blocks, gas_ref, cos_ref, lit_ref, weight_ref, solar_ref, pieces_ref,
    flux_ref, big_ref, state_ref, albedo_ref, cosf_ref, litf_ref,
):
    ncb = cos_ref.shape[0]
    lev = gas_ref.shape[1]
    start_span = lax.axis_index("blk") * (ncb * CB // span)
    expand_weight(weight_ref, big_ref)
    cosf_ref[...] = cos_ref[...].astype(jnp.float32)
    litf_ref[...] = lit_ref[...].astype(jnp.float32)
    direct, diffuse = pick_albedo([pieces_ref[i] for i in range(n)], start_span, span, blocks, ncb)
    albedo_ref[0] = direct
    albedo_ref[1] = diffuse
    solar = solar_column(solar_ref)
    flux_ref[...] = jnp.zeros_like(flux_ref)

    def surface(cb):
        return albedo_ref[0, pl.ds(cb, 1), :], albedo_ref[1, pl.ds(cb, 1), :]

    def one(cb, unused):
        solve_block(
            cb, gas_ref, big_ref, cosf_ref, litf_ref, solar, surface, state_ref, flux_ref,
            round_up(lev + 1, 8),
        )
        return unused

    lax.fori_loop(0, ncb, one, 0)


def side_block(window, centre, picked, weights):
    rows = window.shape[0]
    high = window.astype(jnp.bfloat16)
    low = (window - high.astype(jnp.float32)).astype(jnp.bfloat16)
    both = jnp.concatenate([high, low], axis=0)
    place = lax.broadcasted_iota(jnp.int32, (window.shape[1], CB), 0)
    result = centre
    for k in range(3):
        chosen = (place == picked[k : k + 1]).astype(jnp.float32).astype(jnp.bfloat16)
        beside = jnp.dot(both, chosen, preferred_element_type=jnp.float32)
        result = result + weights[k : k + 1] * (beside[:rows] + beside[rows:] - centre)
    return result


def side_kernel(flux_ref, low_ref, high_ref, neighbours_ref, weights_ref, out_ref, padded_ref):
    cols = flux_ref.shape[1]
    ncb = cols // CB
    interfaces = out_ref.shape[1]
    up_row = round_up(interfaces, 8)
    start = (lax.axis_index("grp") * lax.axis_size("blk") + lax.axis_index("blk")) * cols
    padded_ref[:, 0:CB] = low_ref[...]
    padded_ref[:, CB : CB + cols] = flux_ref[...]
    padded_ref[:, CB + cols :] = high_ref[...]
    for cb in range(ncb):
        own = slice(cb * CB, (cb + 1) * CB)
        picked = neighbours_ref[:, own] - (start + (cb - 1) * CB)
        result = side_block(
            padded_ref[:, cb * CB : (cb + 3) * CB],
            padded_ref[:, (cb + 1) * CB : (cb + 2) * CB],
            picked,
            weights_ref[:, own],
        )
        out_ref[0, :, own] = result[:interfaces]
        out_ref[1, :, own] = result[up_row : up_row + interfaces]


def local(
    gas_state, cos_zenith, daylit, fine_area, fine_albedo, parent_of,
    optics_weight, solar_weight, neighbours, side_weight,
):
    n = lax.axis_size("blk")
    feats, lev, cols = gas_state.shape
    gpoints = solar_weight.shape[0]
    ncb = cols // CB
    blocks = fine_area.shape[0] // FB
    span = cols // blocks
    up_row = round_up(lev + 1, 8)
    half = 16
    full = pl.BlockSpec(memory_space=VMEM)
    pieces = pl.pallas_call(
        functools.partial(albedo_kernel, span),
        out_shape=jax.ShapeDtypeStruct((span + 8, 128), jnp.float32),
        in_specs=[full] * 3,
        out_specs=full,
    )(fine_area.reshape(blocks, FB), fine_albedo, parent_of.reshape(blocks, FB))
    pieces = lax.all_gather(pieces, "blk")
    flux = pl.pallas_call(
        functools.partial(flux_kernel, n, span, blocks),
        out_shape=jax.ShapeDtypeStruct((2 * up_row, cols), jnp.float32),
        in_specs=[full] * 6,
        out_specs=full,
        scratch_shapes=[
            VMEM((half * 2 * gpoints, half * feats), jnp.bfloat16),
            VMEM((4, lev, gpoints, CB), jnp.float32),
            VMEM((2, ncb, CB), jnp.float32),
            VMEM((ncb, CB), jnp.float32),
            VMEM((ncb, CB), jnp.float32),
        ],
    )(
        gas_state, cos_zenith.reshape(ncb, CB), daylit.reshape(ncb, CB), optics_weight,
        solar_weight.reshape(1, gpoints), pieces,
    )
    forward = [(i, i + 1) for i in range(n - 1)]
    backward = [(i + 1, i) for i in range(n - 1)]
    low = lax.ppermute(flux[:, cols - CB :], "blk", forward)
    high = lax.ppermute(flux[:, :CB], "blk", backward)
    return pl.pallas_call(
        side_kernel,
        out_shape=jax.ShapeDtypeStruct((2, lev + 1, cols), jnp.float32),
        in_specs=[full] * 5,
        out_specs=full,
        scratch_shapes=[VMEM((2 * up_row, cols + 2 * CB), jnp.float32)],
    )(flux, low, high, neighbours, side_weight)


def solution(mesh):
    columns = P(("grp", "blk"))
    last = P(None, ("grp", "blk"))
    in_specs = (
        P(None, None, ("grp", "blk")), columns, columns, columns, last, columns, P(), P(), last, last,
    )
    out_specs = P(None, None, ("grp", "blk"))
    return jax.shard_map(local, mesh=mesh, in_specs=in_specs, out_specs=out_specs, check_vma=False)
```

```python
import functools

import jax
import jax.numpy as jnp
from jax import lax
from jax.experimental import pallas as pl
from jax.experimental.pallas import tpu as pltpu
from jax.sharding import PartitionSpec as P

CB = 128
FB = 128
ASYM = 0.8
TAU_SCALE = 0.08
SSA_MAX = 0.98
CHUNK = 8
VMEM = pltpu.VMEM


def round_up(value, multiple):
    return -(-value // multiple) * multiple


def local_albedo(area_ref, albedo_ref, parent_ref, span):
    blocks = area_ref.shape[0]
    area = area_ref[...]
    rows = [
        jnp.concatenate([albedo_ref[s : s + 1, b * FB : (b + 1) * FB] for b in range(blocks)], axis=0)
        for s in range(2)
    ]
    weights = [area, area * rows[0], area * rows[1]]
    weights = [jnp.transpose(w) for w in weights]
    parent = jnp.transpose(parent_ref[...])
    inside = parent & (span - 1)
    sums = [[], [], []]
    for j in range(span):
        hit = inside == j
        for q in range(3):
            sums[q].append(jnp.sum(jnp.where(hit, weights[q], 0.0), axis=0, keepdims=True))
    totals = [jnp.concatenate(s, axis=0) for s in sums]
    first = (totals[1] / totals[0]).astype(jnp.bfloat16).astype(jnp.float32)
    second = (totals[2] / totals[0]).astype(jnp.bfloat16).astype(jnp.float32)
    number = (parent[0:1] // span).astype(jnp.float32)
    return first, second, number


def pick_albedo(pieces, start_span, span, blocks, ncb):
    per = CB // span
    table = jnp.concatenate(
        [jnp.concatenate([p[0:span, s * blocks : (s + 1) * blocks] for p in pieces], axis=1) for s in range(2)],
        axis=0,
    ).astype(jnp.bfloat16)
    number = jnp.concatenate([p[span : span + 1, 0:blocks] for p in pieces], axis=1).astype(jnp.int32)
    total = number.shape[1]
    row = lax.broadcasted_iota(jnp.int32, (ncb, total), 0) * per + start_span
    parts = []
    for m in range(per):
        chosen = (number == row + m).astype(jnp.float32).astype(jnp.bfloat16)
        parts.append(
            lax.dot_general(chosen, table, (((1,), (1,)), ((), ())), preferred_element_type=jnp.float32)
        )
    direct = jnp.concatenate([p[:, 0:span] for p in parts], axis=1)
    diffuse = jnp.concatenate([p[:, span : 2 * span] for p in parts], axis=1)
    return direct, diffuse


def expand_weight(weight_ref, big_ref):
    feats, rows = weight_ref.shape
    half = big_ref.shape[1] // feats
    wide = feats * half
    source = lax.broadcasted_iota(jnp.int32, (feats, wide), 0)
    column = lax.broadcasted_iota(jnp.int32, (feats, wide), 1)
    spread = (column // half == source).astype(jnp.float32).astype(jnp.bfloat16)
    repeated = lax.dot_general(
        weight_ref[...], spread, (((0,), (0,)), ((), ())), preferred_element_type=jnp.float32
    )
    level = lax.broadcasted_iota(jnp.int32, (rows, wide), 1) % half
    for l in range(half):
        big_ref[l * rows : (l + 1) * rows, :] = jnp.where(level == l, repeated, 0.0).astype(jnp.bfloat16)


def layer(mix, gpoints, rate, back, carry):
    direct, big_b, big_q = carry
    x = mix[:gpoints]
    y = mix[gpoints:]
    soft = jnp.maximum(x, 0.0) + jnp.log(1.0 + jnp.exp(-jnp.abs(x)))
    share = jnp.exp(soft * rate)
    th = jnp.tanh(0.5 * y)
    h = 0.5 * SSA_MAX
    w = h + h * th
    up1 = 1.25 + 0.75 * ASYM
    g1 = 2.0 - up1 * w
    c2 = 0.75 * (1.0 - ASYM)
    g2 = c2 * w
    minus = 2.0 - (up1 + c2) * w
    plus = 2.0 - (up1 - c2) * w
    square = minus * plus
    k = square * lax.rsqrt(square)
    q = jnp.exp((k * soft) * (-TAU_SCALE))
    q2 = q * q
    kp = k + g1
    km = k - g1
    d = kp + km * q2
    dd = km + kp * q2
    r = g2 - g2 * q2
    t2 = (k + k) * q
    below = direct * share
    scattered = w * (direct - below)
    rising = scattered * back
    falling = scattered - rising
    z = 1.0 / (d - r * big_b)
    t = t2 * z
    s = (r * big_q + d * rising) * z
    new_b = (r + dd * big_b) * z
    new_q = t * (big_q + big_b * rising) + falling
    return t, s, (below, new_b, new_q)


def descend(cb, gas_ref, big_ref, cos_ref, solar, state_ref, end_ref):
    feats, lev = gas_ref.shape[0], gas_ref.shape[1]
    gpoints = solar.shape[0]
    rows = 2 * gpoints
    half = big_ref.shape[1] // feats
    cols = pl.ds(pl.multiple_of(cb * CB, CB), CB)
    mu = cos_ref[pl.ds(cb, 1), :]
    rate = jnp.broadcast_to(-TAU_SCALE / mu, (gpoints, CB))
    back = jnp.broadcast_to(0.5 * (1.0 - ASYM * mu), (gpoints, CB))
    top = solar * mu
    zero = jnp.zeros((gpoints, CB), jnp.float32)
    carry = (top, zero, zero)

    for part in range(lev // half):
        inputs = gas_ref[:, part * half : (part + 1) * half, cols].reshape(feats * half, CB)

        def down(step, carry, part=part, inputs=inputs):
            at = pl.multiple_of(step * (CHUNK * rows), CHUNK * rows)
            mix = jnp.dot(
                big_ref[pl.ds(at, CHUNK * rows), :], inputs, preferred_element_type=jnp.float32
            )
            for i in range(CHUNK):
                level = part * half + step * CHUNK + i
                state_ref[2, level] = carry[1]
                state_ref[3, level] = carry[2] + carry[0]
                t, s, carry = layer(mix[i * rows : (i + 1) * rows], gpoints, rate, back, carry)
                state_ref[0, level] = t
                state_ref[1, level] = s
            return carry

        carry = lax.fori_loop(0, half // CHUNK, down, carry)
    for i in range(3):
        end_ref[i] = carry[i]


def ascend(cb, albedo_ref, lit_ref, state_ref, end_ref, flux_ref):
    lev = state_ref.shape[1]
    lit = lit_ref[pl.ds(cb, 1), :]
    direct, big_b, big_q = end_ref[0], end_ref[1], end_ref[2]
    direct_albedo = albedo_ref[0, pl.ds(cb, 1), :]
    diffuse_albedo = albedo_ref[1, pl.ds(cb, 1), :]
    up = (diffuse_albedo * big_q + direct_albedo * direct) / (1.0 - diffuse_albedo * big_b)
    last = [
        jnp.sum(big_b * up + big_q + direct, axis=0, keepdims=True) * lit,
        jnp.sum(up, axis=0, keepdims=True) * lit,
        jnp.zeros((flux_ref.shape[0] - 2 * lev - 2, CB), jnp.float32),
    ]
    flux_ref[2 * lev :, :] = jnp.concatenate(last, axis=0)

    def back_up(step, up):
        first = pl.multiple_of(lev - CHUNK - step * CHUNK, CHUNK)
        sums = [None] * (2 * CHUNK)
        for i in reversed(range(CHUNK)):
            up = state_ref[0, first + i] * up + state_ref[1, first + i]
            down = state_ref[2, first + i] * up + state_ref[3, first + i]
            sums[2 * i] = jnp.sum(down, axis=0, keepdims=True)
            sums[2 * i + 1] = jnp.sum(up, axis=0, keepdims=True)
        flux_ref[pl.ds(pl.multiple_of(2 * first, 2 * CHUNK), 2 * CHUNK), :] = jnp.concatenate(sums, axis=0) * lit
        return up

    lax.fori_loop(0, lev // CHUNK, back_up, up)


def solar_column(solar_ref):
    row = solar_ref[...]
    n = row.shape[1]
    diagonal = lax.broadcasted_iota(jnp.int32, (n, n), 0) == lax.broadcasted_iota(jnp.int32, (n, n), 1)
    return jnp.sum(jnp.where(diagonal, row, 0.0), axis=1, keepdims=True)


def flux_kernel(
    n, span, gas_ref, cos_ref, lit_ref, weight_ref, solar_ref, area_ref, fine_albedo_ref, parent_ref,
    flux_ref, big_ref, state_ref, end_ref, albedo_ref, cosf_ref, litf_ref, mine_ref, pieces_ref,
    edge_ref, halo_ref, send_sem, recv_sem, edge_send, edge_recv,
):
    ncb = cos_ref.shape[0]
    blocks = area_ref.shape[0]
    me = lax.axis_index("blk")
    peers = [lax.rem(me + shift, n) for shift in range(1, n)]
    mesh_id = pl.DeviceIdType.MESH

    barrier = pltpu.get_barrier_semaphore()
    for peer in peers:
        pl.semaphore_signal(barrier, inc=1, device_id={"blk": peer}, device_id_type=mesh_id)

    first, second, number = local_albedo(area_ref, fine_albedo_ref, parent_ref, span)
    mine_ref[...] = jnp.zeros_like(mine_ref)
    mine_ref[0:span, 0:blocks] = first
    mine_ref[0:span, blocks : 2 * blocks] = second
    mine_ref[span : span + 1, 0:blocks] = number
    expand_weight(weight_ref, big_ref)
    cosf_ref[...] = cos_ref[...].astype(jnp.float32)
    litf_ref[...] = lit_ref[...].astype(jnp.float32)
    solar = solar_column(solar_ref)

    pl.semaphore_wait(barrier, n - 1)
    sends = []
    for i, peer in enumerate(peers):
        copy = pltpu.make_async_remote_copy(
            src_ref=mine_ref,
            dst_ref=pieces_ref.at[i],
            send_sem=send_sem.at[i],
            recv_sem=recv_sem.at[i],
            device_id={"blk": peer},
            device_id_type=mesh_id,
        )
        copy.start()
        sends.append(copy)

    def edge_down(i, unused):
        descend(i * (ncb - 1), gas_ref, big_ref, cosf_ref, solar, state_ref.at[i], end_ref.at[i])
        return unused

    lax.fori_loop(0, 2, edge_down, 0)
    for copy in sends:
        copy.wait()
    start_span = me * (ncb * CB // span)
    pieces = [mine_ref[...]] + [pieces_ref[i] for i in range(n - 1)]
    direct, diffuse = pick_albedo(pieces, start_span, span, blocks, ncb)
    albedo_ref[0] = direct
    albedo_ref[1] = diffuse

    def edge_up(i, unused):
        ascend(i * (ncb - 1), albedo_ref, litf_ref, state_ref.at[i], end_ref.at[i], edge_ref.at[i])
        return unused

    lax.fori_loop(0, 2, edge_up, 0)
    sends = []
    for i, peer in ((0, peers[-1]), (1, peers[0])):
        copy = pltpu.make_async_remote_copy(
            src_ref=edge_ref.at[i],
            dst_ref=halo_ref.at[i],
            send_sem=edge_send.at[i],
            recv_sem=edge_recv.at[i],
            device_id={"blk": peer},
            device_id_type=mesh_id,
        )
        copy.start()
        sends.append(copy)
    flux_ref[:, CB : 2 * CB] = edge_ref[0]
    flux_ref[:, ncb * CB : (ncb + 1) * CB] = edge_ref[1]

    def one(cb, unused):
        own = pl.ds(pl.multiple_of((cb + 1) * CB, CB), CB)
        descend(cb, gas_ref, big_ref, cosf_ref, solar, state_ref.at[0], end_ref.at[0])
        ascend(cb, albedo_ref, litf_ref, state_ref.at[0], end_ref.at[0], flux_ref.at[:, own])
        return unused

    lax.fori_loop(1, ncb - 1, one, 0)
    for copy in sends:
        copy.wait()
    flux_ref[:, 0:CB] = halo_ref[1]
    flux_ref[:, (ncb + 1) * CB :] = halo_ref[0]


def side_block(window, centre, picked, weights):
    rows = window.shape[0]
    high = window.astype(jnp.bfloat16)
    low = (window - high.astype(jnp.float32)).astype(jnp.bfloat16)
    both = jnp.concatenate([high, low], axis=0)
    place = lax.broadcasted_iota(jnp.int32, (window.shape[1], CB), 0)
    result = centre
    for k in range(3):
        chosen = (place == picked[k : k + 1]).astype(jnp.float32).astype(jnp.bfloat16)
        beside = jnp.dot(both, chosen, preferred_element_type=jnp.float32)
        result = result + weights[k : k + 1] * (beside[:rows] + beside[rows:] - centre)
    return result


def side_kernel(padded_ref, neighbours_ref, weights_ref, out_ref):
    interfaces, parts, cols = out_ref.shape
    ncb = cols // CB
    start = (lax.axis_index("grp") * lax.axis_size("blk") + lax.axis_index("blk")) * cols
    for cb in range(ncb):
        own = slice(cb * CB, (cb + 1) * CB)
        picked = neighbours_ref[:, own] - (start + (cb - 1) * CB)
        result = side_block(
            padded_ref[:, cb * CB : (cb + 3) * CB],
            padded_ref[:, (cb + 1) * CB : (cb + 2) * CB],
            picked,
            weights_ref[:, own],
        )
        out_ref[:, :, own] = result[: parts * interfaces].reshape(interfaces, parts, CB)


def local(
    gas_state, cos_zenith, daylit, fine_area, fine_albedo, parent_of,
    optics_weight, solar_weight, neighbours, side_weight,
):
    n = lax.axis_size("blk")
    feats, lev, cols = gas_state.shape
    gpoints = solar_weight.shape[0]
    ncb = cols // CB
    blocks = fine_area.shape[0] // FB
    span = cols // blocks
    rows = round_up(2 * (lev + 1), 8)
    half = 16
    full = pl.BlockSpec(memory_space=VMEM)
    padded = pl.pallas_call(
        functools.partial(flux_kernel, n, span),
        out_shape=jax.ShapeDtypeStruct((rows, cols + 2 * CB), jnp.float32),
        in_specs=[full] * 8,
        out_specs=full,
        scratch_shapes=[
            VMEM((half * 2 * gpoints, half * feats), jnp.bfloat16),
            VMEM((2, 4, lev, gpoints, CB), jnp.float32),
            VMEM((2, 3, gpoints, CB), jnp.float32),
            VMEM((2, ncb, CB), jnp.float32),
            VMEM((ncb, CB), jnp.float32),
            VMEM((ncb, CB), jnp.float32),
            VMEM((span + 8, 128), jnp.float32),
            VMEM((n - 1, span + 8, 128), jnp.float32),
            VMEM((2, rows, CB), jnp.float32),
            VMEM((2, rows, CB), jnp.float32),
            pltpu.SemaphoreType.DMA((n - 1,)),
            pltpu.SemaphoreType.DMA((n - 1,)),
            pltpu.SemaphoreType.DMA((2,)),
            pltpu.SemaphoreType.DMA((2,)),
        ],
        compiler_params=pltpu.CompilerParams(collective_id=0, has_side_effects=True),
    )(
        gas_state, cos_zenith.reshape(ncb, CB), daylit.reshape(ncb, CB), optics_weight.T,
        solar_weight.reshape(1, gpoints), fine_area.reshape(blocks, FB), fine_albedo,
        parent_of.reshape(blocks, FB),
    )
    result = pl.pallas_call(
        side_kernel,
        out_shape=jax.ShapeDtypeStruct((lev + 1, 2, cols), jnp.float32),
        in_specs=[full] * 3,
        out_specs=full,
    )(padded, neighbours, side_weight)
    return jnp.transpose(result, (1, 0, 2))


def solution(mesh):
    columns = P(("grp", "blk"))
    last = P(None, ("grp", "blk"))
    in_specs = (
        P(None, None, ("grp", "blk")), columns, columns, columns, last, columns, P(), P(), last, last,
    )
    out_specs = P(None, None, ("grp", "blk"))
    return jax.shard_map(local, mesh=mesh, in_specs=in_specs, out_specs=out_specs, check_vma=False)
```

```python
import functools
import math

import jax
import jax.numpy as jnp
from jax import lax
from jax.experimental import pallas as pl
from jax.experimental.pallas import tpu as pltpu
from jax.sharding import PartitionSpec as P

CB = 128
FB = 128
ASYM = 0.8
TAU_SCALE = 0.08
SSA_MAX = 0.98
LOG2E = math.log2(math.e)
CHUNK = 8
VMEM = pltpu.VMEM


def round_up(value, multiple):
    return -(-value // multiple) * multiple


def local_albedo(area_ref, albedo_ref, parent_ref, span):
    blocks = area_ref.shape[0]
    area = area_ref[...]
    rows = [
        jnp.concatenate([albedo_ref[s : s + 1, b * FB : (b + 1) * FB] for b in range(blocks)], axis=0)
        for s in range(2)
    ]
    weights = jnp.transpose(jnp.concatenate([area, area * rows[0], area * rows[1]], axis=0))
    parent = jnp.transpose(jnp.concatenate([parent_ref[...]] * 3, axis=0))
    inside = parent & (span - 1)
    totals = jnp.concatenate(
        [jnp.sum(jnp.where(inside == j, weights, 0.0), axis=0, keepdims=True) for j in range(span)], axis=0
    )
    share = totals[:, :blocks]
    first = (totals[:, blocks : 2 * blocks] / share).astype(jnp.bfloat16).astype(jnp.float32)
    second = (totals[:, 2 * blocks :] / share).astype(jnp.bfloat16).astype(jnp.float32)
    number = (parent[0:1, :blocks] // span).astype(jnp.float32)
    return first, second, number


def pick_albedo(pieces, start_span, span, blocks, ncb):
    per = CB // span
    table = jnp.concatenate(
        [jnp.concatenate([p[0:span, s * blocks : (s + 1) * blocks] for p in pieces], axis=1) for s in range(2)],
        axis=0,
    ).astype(jnp.bfloat16)
    number = jnp.concatenate([p[span : span + 1, 0:blocks] for p in pieces], axis=1).astype(jnp.int32)
    total = number.shape[1]
    row = lax.broadcasted_iota(jnp.int32, (ncb, total), 0) * per + start_span
    parts = []
    for m in range(per):
        chosen = (number == row + m).astype(jnp.float32).astype(jnp.bfloat16)
        parts.append(
            lax.dot_general(chosen, table, (((1,), (1,)), ((), ())), preferred_element_type=jnp.float32)
        )
    direct = jnp.concatenate([p[:, 0:span] for p in parts], axis=1)
    diffuse = jnp.concatenate([p[:, span : 2 * span] for p in parts], axis=1)
    return direct, diffuse


def expand_weight(weight_ref, big_ref):
    feats, rows = weight_ref.shape
    half = big_ref.shape[1] // feats
    wide = feats * half
    source = lax.broadcasted_iota(jnp.int32, (feats, wide), 0)
    column = lax.broadcasted_iota(jnp.int32, (feats, wide), 1)
    spread = (column // half == source).astype(jnp.float32).astype(jnp.bfloat16)
    repeated = lax.dot_general(
        weight_ref[...], spread, (((0,), (0,)), ((), ())), preferred_element_type=jnp.float32
    )
    row = lax.broadcasted_iota(jnp.int32, (rows, wide), 0)
    repeated = jnp.where(row < rows // 2, repeated, 0.5 * repeated)
    level = lax.broadcasted_iota(jnp.int32, (rows, wide), 1) % half
    for l in range(half):
        big_ref[l * rows : (l + 1) * rows, :] = jnp.where(level == l, repeated, 0.0).astype(jnp.bfloat16)


def layer(mix, gpoints, rate, back, carry):
    direct, big_b, big_q = carry
    x = mix[:gpoints]
    soft = jnp.maximum(x, 0.0) + jnp.log(1.0 + jnp.exp2(jnp.abs(x) * (-LOG2E)))
    below = direct * jnp.exp2(soft * rate)
    swing = (0.5 * SSA_MAX) * jnp.tanh(mix[gpoints:])
    w = swing + 0.5 * SSA_MAX
    absorbed = (1.0 - 0.5 * SSA_MAX) - swing
    g2 = (0.375 * (1.0 - ASYM)) * w
    g1 = absorbed + g2
    square = absorbed * (g1 + g2)
    k = square * lax.rsqrt(square)
    q = jnp.exp2((k * soft) * (-2.0 * TAU_SCALE * LOG2E))
    q2 = q * q
    kp = k + g1
    km = k - g1
    d = kp + km * q2
    dd = km + kp * q2
    r = g2 - g2 * q2
    t2 = (k + k) * q
    scattered = w * (direct - below)
    rising = scattered * back
    falling = scattered - rising
    z = 1.0 / (d - r * big_b)
    t = t2 * z
    s = (r * big_q + d * rising) * z
    new_b = (r + dd * big_b) * z
    new_q = t * (big_q + big_b * rising) + falling
    return t, s, (below, new_b, new_q)


def product(block, part, turn, gas_ref, big_ref, mix_ref):
    feats = gas_ref.shape[0]
    half = big_ref.shape[1] // feats
    rows = mix_ref.shape[1]
    cols = pl.ds(pl.multiple_of(block * CB, CB), CB)
    inputs = gas_ref[:, pl.ds(pl.multiple_of(part * half, half), half), cols].reshape(feats * half, CB)
    weight = big_ref[turn * rows : (turn + 1) * rows, :]
    mix_ref[turn] = jnp.dot(weight, inputs, preferred_element_type=jnp.float32)


def descend(cb, after, gas_ref, big_ref, cos_ref, solar, mix_ref, state_ref, end_ref):
    feats, lev = gas_ref.shape[0], gas_ref.shape[1]
    gpoints = solar.shape[0]
    rows = 2 * gpoints
    half = big_ref.shape[1] // feats
    mu = cos_ref[pl.ds(cb, 1), :]
    rate = jnp.broadcast_to((-TAU_SCALE * LOG2E) / mu, (gpoints, CB))
    back = jnp.broadcast_to(0.5 * (1.0 - ASYM * mu), (gpoints, CB))
    top = solar * mu
    zero = jnp.zeros((gpoints, CB), jnp.float32)
    carry = (top, zero, zero)

    turns = half // CHUNK

    def mixed(block, part, turn):
        product(block, part, turn, gas_ref, big_ref, mix_ref)

    def down(part, carry):
        for turn in range(turns):
            if turn + 1 < turns:
                mixed(cb, part, turn + 1)
            for i in range(CHUNK):
                level = part * half + turn * CHUNK + i
                state_ref[2, level] = carry[1]
                state_ref[3, level] = carry[2] + carry[0]
                mix = mix_ref[turn, i * rows : (i + 1) * rows, :]
                t, s, carry = layer(mix, gpoints, rate, back, carry)
                state_ref[0, level] = t
                state_ref[1, level] = s
            if turn == turns - 2:
                last = part == lev // half - 1
                mixed(jnp.where(last, after, cb), jnp.where(last, 0, part + 1), 0)
        return carry

    carry = lax.fori_loop(0, lev // half, down, carry)
    for i in range(3):
        end_ref[i] = carry[i]


def ascend(cb, albedo_ref, lit_ref, state_ref, end_ref, flux_ref):
    lev = state_ref.shape[1]
    lit = lit_ref[pl.ds(cb, 1), :]
    direct, big_b, big_q = end_ref[0], end_ref[1], end_ref[2]
    direct_albedo = albedo_ref[0, pl.ds(cb, 1), :]
    diffuse_albedo = albedo_ref[1, pl.ds(cb, 1), :]
    up = (diffuse_albedo * big_q + direct_albedo * direct) / (1.0 - diffuse_albedo * big_b)
    last = [
        jnp.sum(big_b * up + big_q + direct, axis=0, keepdims=True) * lit,
        jnp.sum(up, axis=0, keepdims=True) * lit,
        jnp.zeros((flux_ref.shape[0] - 2 * lev - 2, CB), jnp.float32),
    ]
    flux_ref[2 * lev :, :] = jnp.concatenate(last, axis=0)

    def back_up(step, up):
        first = pl.multiple_of(lev - CHUNK - step * CHUNK, CHUNK)
        sums = [None] * (2 * CHUNK)
        for i in reversed(range(CHUNK)):
            up = state_ref[0, first + i] * up + state_ref[1, first + i]
            down = state_ref[2, first + i] * up + state_ref[3, first + i]
            sums[2 * i] = jnp.sum(down, axis=0, keepdims=True)
            sums[2 * i + 1] = jnp.sum(up, axis=0, keepdims=True)
        flux_ref[pl.ds(pl.multiple_of(2 * first, 2 * CHUNK), 2 * CHUNK), :] = jnp.concatenate(sums, axis=0) * lit
        return up

    lax.fori_loop(0, lev // CHUNK, back_up, up)


def solar_column(solar_ref):
    row = solar_ref[...]
    n = row.shape[1]
    diagonal = lax.broadcasted_iota(jnp.int32, (n, n), 0) == lax.broadcasted_iota(jnp.int32, (n, n), 1)
    return jnp.sum(jnp.where(diagonal, row, 0.0), axis=1, keepdims=True)


def flux_kernel(
    n, span, gas_hbm, cos_ref, lit_ref, weight_ref, solar_ref, area_ref, fine_albedo_ref, parent_ref,
    flux_ref, big_ref, state_ref, end_ref, albedo_ref, cosf_ref, litf_ref, mine_ref, pieces_ref,
    edge_ref, halo_ref, mix_ref, gas_ref, send_sem, recv_sem, edge_send, edge_recv, gas_sem,
):
    ncb = cos_ref.shape[0]
    blocks = area_ref.shape[0]
    me = lax.axis_index("blk")
    peers = [lax.rem(me + shift, n) for shift in range(1, n)]
    mesh_id = pl.DeviceIdType.MESH

    load = pltpu.make_async_copy(gas_hbm, gas_ref, gas_sem)
    load.start()
    barrier = pltpu.get_barrier_semaphore()
    for peer in peers:
        pl.semaphore_signal(barrier, inc=1, device_id={"blk": peer}, device_id_type=mesh_id)

    first, second, number = local_albedo(area_ref, fine_albedo_ref, parent_ref, span)
    mine_ref[...] = jnp.zeros_like(mine_ref)
    mine_ref[0:span, 0:blocks] = first
    mine_ref[0:span, blocks : 2 * blocks] = second
    mine_ref[span : span + 1, 0:blocks] = number
    expand_weight(weight_ref, big_ref)
    cosf_ref[...] = cos_ref[...].astype(jnp.float32)
    litf_ref[...] = lit_ref[...].astype(jnp.float32)
    solar = solar_column(solar_ref)

    def order(i):
        return jnp.where(i < 2, i * (ncb - 1), i - 1)

    def down(i, slot):
        after = order(jnp.minimum(i + 1, ncb - 1))
        descend(
            order(i), after, gas_ref, big_ref, cosf_ref, solar, mix_ref, state_ref.at[slot], end_ref.at[slot]
        )

    def up(i, slot, target_ref):
        ascend(order(i), albedo_ref, litf_ref, state_ref.at[slot], end_ref.at[slot], target_ref)

    load.wait()
    product(0, 0, 0, gas_ref, big_ref, mix_ref)

    def early_down(i, unused):
        down(i, i)
        return unused

    lax.fori_loop(0, 1, early_down, 0)
    pl.semaphore_wait(barrier, n - 1)
    sends = []
    for i, peer in enumerate(peers):
        copy = pltpu.make_async_remote_copy(
            src_ref=mine_ref,
            dst_ref=pieces_ref.at[i],
            send_sem=send_sem.at[i],
            recv_sem=recv_sem.at[i],
            device_id={"blk": peer},
            device_id_type=mesh_id,
        )
        copy.start()
        sends.append(copy)

    ahead = state_ref.shape[0]
    lax.fori_loop(1, ahead, early_down, 0)
    for copy in sends:
        copy.wait()
    start_span = me * (ncb * CB // span)
    pieces = [mine_ref[...]] + [pieces_ref[i] for i in range(n - 1)]
    direct, diffuse = pick_albedo(pieces, start_span, span, blocks, ncb)
    albedo_ref[0] = direct
    albedo_ref[1] = diffuse

    def edge_up(i, unused):
        up(i, i, edge_ref.at[i])
        return unused

    lax.fori_loop(0, 2, edge_up, 0)
    sends = []
    for i, peer in ((0, peers[-1]), (1, peers[0])):
        copy = pltpu.make_async_remote_copy(
            src_ref=edge_ref.at[i],
            dst_ref=halo_ref.at[i],
            send_sem=edge_send.at[i],
            recv_sem=edge_recv.at[i],
            device_id={"blk": peer},
            device_id_type=mesh_id,
        )
        copy.start()
        sends.append(copy)
    flux_ref[:, CB : 2 * CB] = edge_ref[0]
    flux_ref[:, ncb * CB : (ncb + 1) * CB] = edge_ref[1]

    def own(i):
        return flux_ref.at[:, pl.ds(pl.multiple_of((order(i) + 1) * CB, CB), CB)]

    def early_up(i, unused):
        up(i, i, own(i))
        return unused

    lax.fori_loop(2, ahead, early_up, 0)

    def one(i, unused):
        down(i, 0)
        up(i, 0, own(i))
        return unused

    lax.fori_loop(ahead, ncb, one, 0)
    for copy in sends:
        copy.wait()
    flux_ref[:, 0:CB] = halo_ref[1]
    flux_ref[:, (ncb + 1) * CB :] = halo_ref[0]


def side_block(window, centre, picked, weights):
    rows = window.shape[0]
    high = window.astype(jnp.bfloat16)
    low = (window - high.astype(jnp.float32)).astype(jnp.bfloat16)
    both = jnp.concatenate([high, low], axis=0)
    place = lax.broadcasted_iota(jnp.int32, (window.shape[1], CB), 0)
    result = centre
    for k in range(3):
        chosen = (place == picked[k : k + 1]).astype(jnp.float32).astype(jnp.bfloat16)
        beside = jnp.dot(both, chosen, preferred_element_type=jnp.float32)
        result = result + weights[k : k + 1] * (beside[:rows] + beside[rows:] - centre)
    return result


def side_kernel(padded_ref, neighbours_ref, weights_ref, out_ref):
    interfaces, parts, cols = out_ref.shape
    ncb = cols // CB
    start = (lax.axis_index("grp") * lax.axis_size("blk") + lax.axis_index("blk")) * cols
    for cb in range(ncb):
        own = slice(cb * CB, (cb + 1) * CB)
        picked = neighbours_ref[:, own] - (start + (cb - 1) * CB)
        result = side_block(
            padded_ref[:, cb * CB : (cb + 3) * CB],
            padded_ref[:, (cb + 1) * CB : (cb + 2) * CB],
            picked,
            weights_ref[:, own],
        )
        out_ref[:, :, own] = result[: parts * interfaces].reshape(interfaces, parts, CB)


def local(
    gas_state, cos_zenith, daylit, fine_area, fine_albedo, parent_of,
    optics_weight, solar_weight, neighbours, side_weight,
):
    n = lax.axis_size("blk")
    feats, lev, cols = gas_state.shape
    gpoints = solar_weight.shape[0]
    ncb = cols // CB
    blocks = fine_area.shape[0] // FB
    span = cols // blocks
    rows = round_up(2 * (lev + 1), 8)
    half = 16
    full = pl.BlockSpec(memory_space=VMEM)
    padded = pl.pallas_call(
        functools.partial(flux_kernel, n, span),
        out_shape=jax.ShapeDtypeStruct((rows, cols + 2 * CB), jnp.float32),
        in_specs=[pl.BlockSpec(memory_space=pl.ANY)] + [full] * 7,
        out_specs=full,
        scratch_shapes=[
            VMEM((half * 2 * gpoints, half * feats), jnp.bfloat16),
            VMEM((4, 4, lev, gpoints, CB), jnp.float32),
            VMEM((4, 3, gpoints, CB), jnp.float32),
            VMEM((2, ncb, CB), jnp.float32),
            VMEM((ncb, CB), jnp.float32),
            VMEM((ncb, CB), jnp.float32),
            VMEM((span + 8, 128), jnp.float32),
            VMEM((n - 1, span + 8, 128), jnp.float32),
            VMEM((2, rows, CB), jnp.float32),
            VMEM((2, rows, CB), jnp.float32),
            VMEM((half // CHUNK, CHUNK * 2 * gpoints, CB), jnp.float32),
            VMEM((feats, lev, cols), gas_state.dtype),
            pltpu.SemaphoreType.DMA((n - 1,)),
            pltpu.SemaphoreType.DMA((n - 1,)),
            pltpu.SemaphoreType.DMA((2,)),
            pltpu.SemaphoreType.DMA((2,)),
            pltpu.SemaphoreType.DMA,
        ],
        compiler_params=pltpu.CompilerParams(collective_id=0, has_side_effects=True),
    )(
        gas_state, cos_zenith.reshape(ncb, CB), daylit.reshape(ncb, CB), optics_weight.T,
        solar_weight.reshape(1, gpoints), fine_area.reshape(blocks, FB), fine_albedo,
        parent_of.reshape(blocks, FB),
    )
    result = pl.pallas_call(
        side_kernel,
        out_shape=jax.ShapeDtypeStruct((lev + 1, 2, cols), jnp.float32),
        in_specs=[full] * 3,
        out_specs=full,
    )(padded, neighbours, side_weight)
    return jnp.transpose(result, (1, 0, 2))


def solution(mesh):
    columns = P(("grp", "blk"))
    last = P(None, ("grp", "blk"))
    in_specs = (
        P(None, None, ("grp", "blk")), columns, columns, columns, last, columns, P(), P(), last, last,
    )
    out_specs = P(None, None, ("grp", "blk"))
    return jax.shard_map(local, mesh=mesh, in_specs=in_specs, out_specs=out_specs, check_vma=False)
```
